32 devices in a mesh: dp: 4 (over y, z), ep: 8 (over x, core).
Axes of the slice: x: 4, y: 2, z: 2, core: 2. Of those that a mesh axis runs over, the one named last changes fastest.
The devices are a block of a 4x4x8 slice.
Arguments:
- hidden: bfloat16 [4096, 2560], P(('dp', 'ep')), parts along dimension 0
- norm_gain: float32 [2560], replicated
- router_w: bfloat16 [2560, 64], replicated
- topk_idx: int32 [4096, 6], P(('dp', 'ep')), parts along dimension 0
- w_gate: bfloat16 [64, 2560, 1536], P('ep')
- w_up: bfloat16 [64, 2560, 1536], P('ep')
- w_down: bfloat16 [64, 1536, 2560], P('ep')
- shared_gate: bfloat16 [2560, 3072], replicated
- shared_up: bfloat16 [2560, 3072], replicated
- shared_down: bfloat16 [3072, 2560], replicated
Outputs:
- output: bfloat16 [4096, 2560], P(('dp', 'ep')), parts along dimension 0
There are 4 independent parts. The reference program is written for one: setup_inputs(seed, part) draws one part's arguments, and reference() takes and returns one part's arrays. A program takes and returns all parts, laid end to end along the dimension named above; an argument that names none is the same for every part.
All inputs are finite; a program needn't handle non-finite values.
Results may differ from the reference program's by a relative error of at most 0.00101.
Values are sent between devices in bfloat16 or wider.
A program may use at most 768 MiB of HBM per device.

```python
import jax
import jax.numpy as jnp
from jax import lax

HIDDEN = 2560
EXPERTS = 64
TOP_K = 6
EXPERT_FF = 1536
SHARED_FF = 3072
GROUP_SIZE = 8
TOKENS = 128
ROW_BLOCK = 128
NORM_EPS = 1e-6

NUM_TOKENS = GROUP_SIZE * TOKENS
ROUTE_ROWS = NUM_TOKENS * TOP_K
NUM_BLOCKS = (ROUTE_ROWS + EXPERTS * (ROW_BLOCK - 1) + ROW_BLOCK - 1) // ROW_BLOCK


def draw_routing(route_key):
    mean_rows = TOKENS * TOP_K // EXPERTS
    half_rows = mean_rows // 2

    def one_device(dev_key):
        key_pair, key_shift, key_layout, key_tokens = jax.random.split(dev_key, 4)
        pair_perm = jax.random.permutation(key_pair, EXPERTS)
        shift_rows = jax.random.randint(key_shift, (EXPERTS // 2,), -half_rows, half_rows + 1)
        shift_rows = shift_rows.at[0].set(half_rows)
        pair_counts = jnp.stack([mean_rows + shift_rows, mean_rows - shift_rows], axis=1).reshape(EXPERTS)
        counts = jnp.zeros((EXPERTS,), jnp.int32).at[pair_perm].set(pair_counts)
        layout_order = jax.random.permutation(key_layout, EXPERTS)
        bounds = jnp.cumsum(counts[layout_order])
        positions = jnp.arange(TOKENS * TOP_K)
        range_index = jnp.sum(positions[:, None] >= bounds[None, :], axis=1)
        expert_grid = layout_order[range_index].reshape(TOP_K, TOKENS)
        token_perm = jax.random.permutation(key_tokens, TOKENS)
        return jnp.zeros((TOKENS, TOP_K), jnp.int32).at[token_perm].set(expert_grid.T)

    dev_keys = jax.random.split(route_key, GROUP_SIZE)
    return jax.vmap(one_device)(dev_keys).reshape(NUM_TOKENS, TOP_K).astype(jnp.int32)


def setup_inputs(seed: int = 0, part: int = 0) -> dict:
    base_key = jax.random.key(seed)
    part_key = jax.random.fold_in(base_key, part)
    key_hidden, key_route = jax.random.split(part_key, 2)
    weight_keys = jax.random.split(base_key, 8)
    in_scale = HIDDEN ** -0.5
    down_scale = (EXPERTS / TOP_K) * EXPERT_FF ** -0.5
    hidden = 0.5 * jax.random.normal(key_hidden, (NUM_TOKENS, HIDDEN), jnp.float32)
    norm_gain = jax.random.uniform(weight_keys[0], (HIDDEN,), jnp.float32, 0.5, 1.5)
    router_w = in_scale * jax.random.normal(weight_keys[1], (HIDDEN, EXPERTS), jnp.float32)
    w_gate = in_scale * jax.random.normal(weight_keys[2], (EXPERTS, HIDDEN, EXPERT_FF), jnp.float32)
    w_up = in_scale * jax.random.normal(weight_keys[3], (EXPERTS, HIDDEN, EXPERT_FF), jnp.float32)
    w_down = down_scale * jax.random.normal(weight_keys[4], (EXPERTS, EXPERT_FF, HIDDEN), jnp.float32)
    shared_gate = in_scale * jax.random.normal(weight_keys[5], (HIDDEN, SHARED_FF), jnp.float32)
    shared_up = in_scale * jax.random.normal(weight_keys[6], (HIDDEN, SHARED_FF), jnp.float32)
    shared_down = 0.5 * SHARED_FF ** -0.5 * jax.random.normal(weight_keys[7], (SHARED_FF, HIDDEN), jnp.float32)
    return {
        'hidden': hidden.astype(jnp.bfloat16),
        'norm_gain': norm_gain,
        'router_w': router_w.astype(jnp.bfloat16),
        'topk_idx': draw_routing(key_route),
        'w_gate': w_gate.astype(jnp.bfloat16),
        'w_up': w_up.astype(jnp.bfloat16),
        'w_down': w_down.astype(jnp.bfloat16),
        'shared_gate': shared_gate.astype(jnp.bfloat16),
        'shared_up': shared_up.astype(jnp.bfloat16),
        'shared_down': shared_down.astype(jnp.bfloat16),
    }


def rms_norm(hidden, norm_gain):
    hidden_f32 = hidden.astype(jnp.float32)
    inv_rms = lax.rsqrt(jnp.mean(hidden_f32 * hidden_f32, axis=-1, keepdims=True) + NORM_EPS)
    return (hidden_f32 * inv_rms * norm_gain).astype(jnp.bfloat16)


def swiglu_rows(rows_in, gate_w, up_w, down_w):
    gate_out = jnp.dot(rows_in, gate_w, preferred_element_type=jnp.float32)
    up_out = jnp.dot(rows_in, up_w, preferred_element_type=jnp.float32)
    activated = (jax.nn.silu(gate_out) * up_out).astype(jnp.bfloat16)
    return jnp.dot(activated, down_w, preferred_element_type=jnp.float32)


def reference(hidden, norm_gain, router_w, topk_idx, w_gate, w_up, w_down, shared_gate, shared_up, shared_down):
    normed = rms_norm(hidden, norm_gain)
    logits = jnp.dot(normed, router_w, preferred_element_type=jnp.float32)
    route_w = jnp.take_along_axis(jax.nn.softmax(logits, axis=-1), topk_idx, axis=1)
    shared_out = swiglu_rows(normed, shared_gate, shared_up, shared_down)
    flat_expert = topk_idx.reshape(-1)
    row_order = jnp.argsort(flat_expert, stable=True)
    sorted_expert = flat_expert[row_order]
    counts = jnp.zeros((EXPERTS,), jnp.int32).at[flat_expert].add(1)
    padded = (counts + ROW_BLOCK - 1) // ROW_BLOCK * ROW_BLOCK
    sorted_start = jnp.cumsum(counts) - counts
    padded_end = jnp.cumsum(padded)
    padded_start = padded_end - padded
    dest_sorted = padded_start[sorted_expert] + jnp.arange(ROUTE_ROWS) - sorted_start[sorted_expert]
    slot_token = jnp.full((NUM_BLOCKS * ROW_BLOCK,), NUM_TOKENS, jnp.int32).at[dest_sorted].set(row_order // TOP_K)
    dest_of_row = jnp.zeros((ROUTE_ROWS,), jnp.int32).at[row_order].set(dest_sorted)
    block_first = jnp.arange(NUM_BLOCKS) * ROW_BLOCK
    block_expert = jnp.minimum(jnp.sum(block_first[:, None] >= padded_end[None, :], axis=1), EXPERTS - 1)
    normed_pad = jnp.concatenate([normed, jnp.zeros((1, HIDDEN), normed.dtype)], axis=0)
    block_rows = normed_pad[slot_token].reshape(NUM_BLOCKS, ROW_BLOCK, HIDDEN)

    def one_block(block_in):
        block_x, expert_id = block_in
        expert_out = swiglu_rows(block_x, w_gate[expert_id], w_up[expert_id], w_down[expert_id])
        return expert_out.astype(jnp.bfloat16)

    padded_out = lax.map(one_block, (block_rows, block_expert)).reshape(NUM_BLOCKS * ROW_BLOCK, HIDDEN)
    row_out = padded_out[dest_of_row].reshape(NUM_TOKENS, TOP_K, HIDDEN)
    routed = jnp.sum(row_out.astype(jnp.float32) * route_w[:, :, None], axis=1)
    return (hidden.astype(jnp.float32) + shared_out + routed).astype(jnp.bfloat16)
```

```python
import functools

import jax
import jax.numpy as jnp
from jax import lax
from jax.experimental import pallas as pl
from jax.experimental.pallas import tpu as pltpu
from jax.sharding import PartitionSpec as P

NORM_EPS = 1e-6
MESH = pl.DeviceIdType.MESH
F32 = jnp.float32
BF16 = jnp.bfloat16
MAIN = 16
GU_SLOTS = 4
D_SLOTS = 4
FF_CHUNKS = 3
H_CHUNKS = 2


def dot(a, b):
    return jnp.dot(a, b, preferred_element_type=F32)


def iota(shape, axis):
    return lax.broadcasted_iota(jnp.int32, shape, axis)


def moe_kernel(
    group, x_hbm, gain_ref, rw_ref, topk_ref, wg, wu, wd, sg, su, sd, out_hbm,
    gx, xo, back, tail, gu_buf, d_buf, act, normed, acc, w_stack, code_all, sel_tail, out_v,
    x_sem, gu_sem, d_sem, xs_sem, xr_sem, cs_sem, cr_sem, os_sem, or_sem,
):
    tok, hid = x_hbm.shape
    ff = wg.shape[2]
    local = wg.shape[0]
    experts = rw_ref.shape[1]
    rounds = local + 1
    fc, hc = ff // FF_CHUNKS, hid // H_CHUNKS
    shared_units = sg.shape[1] // ff
    half = tok // 2
    chips = group // 2

    me = lax.axis_index("ep")
    chip, core = me // 2, me % 2

    def dev(chip_off, flip):
        return ((chip + chip_off) % chips) * 2 + (core + flip) % 2

    def gu_copies(unit, f, slot, shared):
        if shared:
            cols = pl.ds(pl.multiple_of(unit * ff + f * fc, 128), fc)
            srcs = (sg.at[:, cols], su.at[:, cols])
        else:
            cols = pl.ds(f * fc, fc)
            srcs = (wg.at[unit, :, cols], wu.at[unit, :, cols])
        return [pltpu.make_async_copy(srcs[m], gu_buf.at[slot, m], gu_sem.at[slot, m]) for m in range(2)]

    def d_copy(unit, h, slot, shared):
        cols = pl.ds(h * hc, hc)
        src = sd.at[pl.ds(pl.multiple_of(unit * ff, 16), ff), cols] if shared else wd.at[unit, :, cols]
        return pltpu.make_async_copy(src, d_buf.at[slot], d_sem.at[slot])

    def start_gu(unit, f, slot, shared):
        for copy in gu_copies(unit, f, slot, shared):
            copy.start()

    x_copy = pltpu.make_async_copy(x_hbm, gx.at[me], x_sem)
    x_copy.start()
    for q in range(GU_SLOTS):
        start_gu(q // FF_CHUNKS, q % FF_CHUNKS, q, True)
        if q < D_SLOTS:
            d_copy(q // H_CHUNKS, q % H_CHUNKS, q, True).start()

    barrier = pltpu.get_barrier_semaphore()
    for r in range(1, group):
        pl.semaphore_signal(barrier, inc=1, device_id={"ep": (me + r) % group}, device_id_type=MESH)
    pl.semaphore_wait(barrier, group - 1)

    def x_send(src, part, dst, slot):
        rows = gx.at[src, pl.ds(part * half, half)]
        return pltpu.make_async_remote_copy(
            src_ref=rows, dst_ref=rows, send_sem=xs_sem.at[slot], recv_sem=xr_sem.at[src, part],
            device_id={"ep": dst}, device_id_type=MESH)

    def x_wait(src, part):
        x_send(src, part, me, 0).wait_recv()

    left, right, far, partner = dev(chips - 1, 0), dev(1, 0), dev(2, 0), dev(0, 1)
    x_copy.wait()
    x_sends = [
        (me, 0, right), (me, 1, left), (me, 1, right), (me, 0, left), (me, 0, partner), (me, 1, partner),
        (left, 0, right), (left, 0, partner), (right, 1, left), (right, 1, partner),
        (left, 1, partner), (right, 0, partner), (far, 0, partner), (far, 1, partner),
    ]

    def start_x(lo, hi):
        for slot in range(lo, hi):
            x_send(*x_sends[slot], slot).start()

    start_x(0, 6)

    topk = topk_ref[...]
    lanes = iota((tok, 128), 1)
    chosen = jnp.zeros((tok, 128), F32)
    for j in range(topk.shape[1]):
        chosen = jnp.where(topk[:, j:j + 1] == lanes, 1.0, chosen)
    before = jnp.where(iota((tok, tok), 1) < iota((tok, tok), 0), 1.0, 0.0).astype(BF16)
    code = jnp.where(chosen > 0.5, dot(before, chosen.astype(BF16)), -1.0)
    code_t = code.T[:experts]
    code_all[me] = code_t.reshape(group, local, tok)

    def code_send(dst, r):
        return pltpu.make_async_remote_copy(
            src_ref=code_all.at[me, dst], dst_ref=code_all.at[me, dst], send_sem=cs_sem.at[r], recv_sem=cr_sem.at[me],
            device_id={"ep": dst}, device_id_type=MESH)

    def code_wait(src):
        pltpu.make_async_remote_copy(
            src_ref=code_all.at[src, me], dst_ref=code_all.at[src, me], send_sem=cs_sem.at[0], recv_sem=cr_sem.at[src],
            device_id={"ep": me}, device_id_type=MESH).wait_recv()

    def norm(rows_f32):
        inv_rms = lax.rsqrt(jnp.mean(rows_f32 * rows_f32, axis=-1, keepdims=True) + NORM_EPS)
        return (rows_f32 * inv_rms * gain_ref[...]).astype(BF16)

    x_own = gx[me].astype(F32)
    normed[...] = norm(x_own)
    acc[...] = x_own
    for r in range(1, group):
        code_send((me + r) % group, r).start()

    def unit_step(rows, load_rows, gu_first, d_first, next_gu, next_d, put_out):
        for f in range(FF_CHUNKS):
            slot = (gu_first + f) % GU_SLOTS
            for copy in gu_copies(0, 0, slot, False):
                copy.wait()
            gate = dot(load_rows(), gu_buf[slot, 0])
            up = dot(load_rows(), gu_buf[slot, 1])
            act[pl.ds(0, rows), pl.ds(f * fc, fc)] = (jax.nn.silu(gate) * up).astype(BF16)
            next_gu(f, slot)
        for h in range(H_CHUNKS):
            slot = (d_first + h) % D_SLOTS
            d_copy(0, 0, slot, False).wait()
            put_out(h, dot(act[pl.ds(0, rows), :], d_buf[slot]))
            next_d(h, slot)

    def shared_step(u, carry):
        def next_gu(f, slot):
            ahead = (f + GU_SLOTS) // FF_CHUNKS
            f_next = (f + GU_SLOTS) % FF_CHUNKS

            @pl.when(u + ahead < shared_units)
            def _():
                start_gu(u + ahead, f_next, slot, True)

            @pl.when(u + ahead >= shared_units)
            def _():
                start_gu(u + ahead - shared_units, f_next, slot, False)

        def next_d(h, slot):
            d_copy(u + D_SLOTS // H_CHUNKS - shared_units, h, slot, False).start()

        def put_out(h, value):
            cols = pl.ds(h * hc, hc)
            acc[:, cols] = acc[:, cols] + value

        unit_step(tok, lambda: normed[...], u * FF_CHUNKS, u * H_CHUNKS, next_gu, next_d, put_out)

        @pl.when(u == 0)
        def _():
            x_wait(left, 0)
            start_x(6, 8)
            x_wait(right, 1)
            start_x(8, 10)

        return carry

    lax.fori_loop(0, shared_units, shared_step, 0)
    x_wait(left, 1)
    start_x(10, 11)
    x_wait(right, 0)
    start_x(11, 12)

    logits = dot(normed[...], rw_ref[...])
    peak = jnp.max(logits, axis=-1, keepdims=True)
    grown = jnp.exp(logits - peak)
    probs = grown / jnp.sum(grown, axis=-1, keepdims=True)
    p_hi = probs.astype(BF16)
    rest = probs - p_hi.astype(F32)
    p_mid = rest.astype(BF16)
    p_low = (rest - p_mid.astype(F32)).astype(BF16)
    spread_in = jnp.concatenate([code[:, :experts].astype(BF16), p_hi, p_mid, p_low], axis=0)

    def slot_weights(i, carry):
        lane = iota((1, group * MAIN), 1)
        owner, place = lane // MAIN, lane % MAIN
        extra = MAIN // local
        last = jnp.full((1, group * MAIN), i, jnp.int32) == local
        expert = owner * local + jnp.where(last, place // extra, i)
        rank = jnp.where(last, MAIN + place % extra, place).astype(F32)
        pick = jnp.where(iota((experts, group * MAIN), 0) == expert, 1.0, 0.0).astype(BF16)
        spread = dot(spread_in, pick)
        hit = spread[:tok] == rank
        for part in range(3):
            value = jnp.where(hit, spread[(part + 1) * tok:(part + 2) * tok], 0.0)
            w_stack[i, pl.ds(part * tok, tok), :] = value.astype(BF16)
        return carry

    lax.fori_loop(0, rounds, slot_weights, 0)

    def gather_owner(src):
        codes = code_all[src, me]
        spread = jnp.broadcast_to(codes[:, None, :], (local, MAIN, tok)).reshape(local * MAIN, tok)
        row = iota((local * MAIN, tok), 0)
        place = row % MAIN
        pick = jnp.where(spread == place.astype(F32), 1.0, 0.0).astype(BF16)
        extra = MAIN // local
        want = jnp.where(place // extra == src, MAIN + place % extra, -2).astype(F32)
        sel_tail[src] = jnp.where(spread == want, 1.0, 0.0).astype(BF16)
        rows = norm(dot(pick, gx[src]))
        xo[:, src] = rows.reshape(local, MAIN, hid)

    code_all_waits = [dev(off, flip) for off in range(chips) for flip in range(2) if (off, flip) != (0, 0)]
    for src in code_all_waits:
        code_wait(src)
    for off in (0, 1, chips - 1):
        for part in range(2):
            x_wait(dev(off, 1), part)

    def gather_near(p, carry):
        q = p // 2
        gather_owner(dev(q * (q + 1) // 2, p % 2))
        return carry

    lax.fori_loop(0, 6, gather_near, 0)
    x_wait(far, 0)
    start_x(12, 13)
    x_wait(far, 1)
    start_x(13, 14)
    for part in range(2):
        x_wait(dev(2, 1), part)

    def gather_far(p, carry):
        gather_owner(dev(2, p))
        return carry

    lax.fori_loop(0, 2, gather_far, 0)
    picks = jnp.concatenate([sel_tail[s] for s in range(group)], axis=1)
    rows = norm(dot(picks, gx[...].reshape(group * tok, hid)))
    xo[:, group] = rows.reshape(local, MAIN, hid)

    order = [(2, 0), (2, 1), (1, 0), (chips - 1, 0), (1, 1), (chips - 1, 1), (0, 1)]

    def back_send(i, src_ref, slot, dst):
        return pltpu.make_async_remote_copy(
            src_ref=src_ref, dst_ref=back.at[i, me], send_sem=os_sem.at[i, slot], recv_sem=or_sem.at[i, me],
            device_id={"ep": dst}, device_id_type=MESH)

    def back_wait(i, src):
        pltpu.make_async_remote_copy(
            src_ref=back.at[i, src], dst_ref=back.at[i, src], send_sem=os_sem.at[0, 0], recv_sem=or_sem.at[i, src],
            device_id={"ep": me}, device_id_type=MESH).wait_recv()

    def combine(i):
        for off, flip in order:
            back_wait(i, dev(off, flip))
        for h in range(H_CHUNKS):
            cols = pl.ds(h * hc, hc)
            parts = dot(w_stack[i], back[i, :, :, cols].reshape(group * MAIN, hc))
            acc[:, cols] = acc[:, cols] + (parts[:tok] + (parts[tok:2 * tok] + parts[2 * tok:]))

    def routed_step(i, carry):
        rows = (group + 1) * MAIN

        def next_gu(f, slot):
            ahead = (f + GU_SLOTS) // FF_CHUNKS
            f_next = (f + GU_SLOTS) % FF_CHUNKS

            @pl.when(i + ahead < local)
            def _():
                start_gu(i + ahead, f_next, slot, False)

        def next_d(h, slot):
            ahead = D_SLOTS // H_CHUNKS

            @pl.when(i + ahead < local)
            def _():
                d_copy(i + ahead, h, slot, False).start()

        def put_out(h, value):
            xo[i, :, :, pl.ds(h * hc, hc)] = value.astype(BF16).reshape(group + 1, MAIN, hc)

        unit_step(
            rows, lambda: xo[i].reshape(rows, hid), (i + shared_units) * FF_CHUNKS, (i + shared_units) * H_CHUNKS,
            next_gu, next_d, put_out)
        for slot, (off, flip) in enumerate(order):
            dst = dev(off, flip)
            back_send(i, xo.at[i, dst], slot, dst).start()
        back[i, me] = xo[i, me]

        @pl.when(i >= 2)
        def _():
            combine(i - 2)

        return carry

    lax.fori_loop(0, local, routed_step, 0)

    left_over = xo[:, group].reshape(local * MAIN, hid)
    row, col = iota((local * MAIN, local * MAIN), 0), iota((local * MAIN, local * MAIN), 1)
    extra = MAIN // local
    source = ((row % MAIN) // extra) * MAIN + (row // MAIN) * extra + row % extra
    reorder = jnp.where(col == source, 1.0, 0.0).astype(BF16)
    tail[...] = dot(reorder, left_over).astype(BF16).reshape(group, MAIN, hid)
    for slot, (off, flip) in enumerate(order):
        dst = dev(off, flip)
        back_send(local, tail.at[dst], slot, dst).start()
    back[local, me] = tail[me]

    def combine_step(i, carry):
        combine(i)
        return carry

    lax.fori_loop(local - 2, rounds, combine_step, 0)
    out_v[...] = acc[...].astype(BF16)
    out_copy = pltpu.make_async_copy(out_v, out_hbm, x_sem)
    out_copy.start()

    for slot in range(len(x_sends)):
        x_send(*x_sends[slot], slot).wait_send()
    for r in range(1, group):
        code_send((me + r) % group, r).wait_send()

    def drain(i, carry):
        for slot, (off, flip) in enumerate(order):
            dst = dev(off, flip)
            back_send(i, tail.at[dst], slot, dst).wait_send()
        return carry

    lax.fori_loop(0, rounds, drain, 0)
    out_copy.wait()


def solution(mesh):
    group = mesh.shape["ep"]

    def local_step(hidden, norm_gain, router_w, topk_idx, w_gate, w_up, w_down, shared_gate, shared_up, shared_down):
        tok, hid = hidden.shape
        top_k = topk_idx.shape[1]
        experts = router_w.shape[1]
        local, _, ff = w_gate.shape
        capacity = 3 * tok * top_k // (2 * experts)
        assert group == 8 and (capacity - MAIN) * local == MAIN and local == group
        rounds = local + 1
        fc, hc = ff // FF_CHUNKS, hid // H_CHUNKS
        any_spec = pl.BlockSpec(memory_space=pl.ANY)
        vmem_spec = pl.BlockSpec(memory_space=pltpu.VMEM)
        dma = pltpu.SemaphoreType.DMA
        return pl.pallas_call(
            functools.partial(moe_kernel, group),
            out_shape=jax.ShapeDtypeStruct((tok, hid), BF16),
            in_specs=[any_spec, vmem_spec, vmem_spec, vmem_spec] + [any_spec] * 6,
            out_specs=any_spec,
            scratch_shapes=[
                pltpu.VMEM((group, tok, hid), BF16),
                pltpu.VMEM((local, group + 1, MAIN, hid), BF16),
                pltpu.VMEM((rounds, group, MAIN, hid), BF16),
                pltpu.VMEM((group, MAIN, hid), BF16),
                pltpu.VMEM((GU_SLOTS, 2, hid, fc), BF16),
                pltpu.VMEM((D_SLOTS, ff, hc), BF16),
                pltpu.VMEM(((group + 1) * MAIN, ff), BF16),
                pltpu.VMEM((tok, hid), BF16),
                pltpu.VMEM((tok, hid), F32),
                pltpu.VMEM((rounds, 3 * tok, group * MAIN), BF16),
                pltpu.VMEM((group, group, local, tok), F32),
                pltpu.VMEM((group, local * MAIN, tok), BF16),
                pltpu.VMEM((tok, hid), BF16),
                dma,
                dma((GU_SLOTS, 2)),
                dma((D_SLOTS,)),
                dma((14,)),
                dma((group, 2)),
                dma((group,)),
                dma((group,)),
                dma((rounds, group - 1)),
                dma((rounds, group)),
            ],
            compiler_params=pltpu.CompilerParams(
                collective_id=0, has_side_effects=True, vmem_limit_bytes=67_000_000),
            name="moe_block",
        )(hidden, norm_gain.reshape(1, hid), router_w, topk_idx, w_gate, w_up, w_down, shared_gate, shared_up, shared_down)

    token_spec = P(("dp", "ep"), None)
    expert_spec = P("ep", None, None)
    return jax.shard_map(
        local_step,
        mesh=mesh,
        in_specs=(token_spec, P(None), P(None, None), token_spec, expert_spec, expert_spec, expert_spec,
                  P(None, None), P(None, None), P(None, None)),
        out_specs=token_spec,
        check_vma=False,
    )
```

```python
import functools

import jax
import jax.numpy as jnp
from jax import lax
from jax.experimental import pallas as pl
from jax.experimental.pallas import tpu as pltpu
from jax.sharding import PartitionSpec as P

NORM_EPS = 1e-6
MESH = pl.DeviceIdType.MESH
F32 = jnp.float32
BF16 = jnp.bfloat16
MAIN = 16
GU_SLOTS = 4
D_SLOTS = 4
FF_CHUNKS = 3
H_CHUNKS = 2


def dot(a, b):
    return jnp.dot(a, b, preferred_element_type=F32)


def iota(shape, axis):
    return lax.broadcasted_iota(jnp.int32, shape, axis)


def moe_kernel(
    group, x_hbm, gain_hbm, rw_hbm, topk_hbm, wg, wu, wd, sg, su, sd, out_hbm,
    gx, xo, back, tail, gu_buf, d_buf, act, normed, acc, w_stack, code_all, sel_tail, tail_sum,
    gain_ref, rw_ref, topk_ref, in_sem, x_sem, gu_sem, d_sem, xs_sem, xr_sem, cs_sem, cr_sem, os_sem, or_sem,
):
    tok, hid = x_hbm.shape
    ff = wg.shape[2]
    local = wg.shape[0]
    experts = rw_hbm.shape[0]
    rounds = local + 1
    fc, hc = ff // FF_CHUNKS, hid // H_CHUNKS
    shared_units = sg.shape[1] // ff
    half = tok // 2
    chips = group // 2

    me = lax.axis_index("ep")
    chip, core = me // 2, me % 2

    def dev(chip_off, flip):
        return ((chip + chip_off) % chips) * 2 + (core + flip) % 2

    def gu_copies(unit, f, slot, shared):
        if shared:
            cols = pl.ds(pl.multiple_of(unit * ff + f * fc, 128), fc)
            srcs = (sg.at[:, cols], su.at[:, cols])
        else:
            cols = pl.ds(f * fc, fc)
            srcs = (wg.at[unit, :, cols], wu.at[unit, :, cols])
        return [pltpu.make_async_copy(srcs[m], gu_buf.at[slot, m], gu_sem.at[slot, m]) for m in range(2)]

    def d_copy(unit, h, slot, shared):
        cols = pl.ds(h * hc, hc)
        src = sd.at[pl.ds(pl.multiple_of(unit * ff, 16), ff), cols] if shared else wd.at[unit, :, cols]
        return pltpu.make_async_copy(src, d_buf.at[slot], d_sem.at[slot])

    def start_gu(unit, f, slot, shared):
        for copy in gu_copies(unit, f, slot, shared):
            copy.start()

    x_copy = pltpu.make_async_copy(x_hbm, gx.at[me], x_sem)
    x_copy.start()
    small = [
        pltpu.make_async_copy(topk_hbm, topk_ref, in_sem.at[0]),
        pltpu.make_async_copy(gain_hbm, gain_ref, in_sem.at[1]),
        pltpu.make_async_copy(rw_hbm, rw_ref, in_sem.at[2]),
    ]
    for copy in small:
        copy.start()

    barrier = pltpu.get_barrier_semaphore()
    for r in range(1, group):
        pl.semaphore_signal(barrier, inc=1, device_id={"ep": (me + r) % group}, device_id_type=MESH)
    x_copy.wait()
    for q in range(GU_SLOTS):
        start_gu(q // FF_CHUNKS, q % FF_CHUNKS, q, True)
        if q < D_SLOTS:
            d_copy(q // H_CHUNKS, q % H_CHUNKS, q, True).start()

    for copy in small:
        copy.wait()
    line = iota((tok, tok), 0)
    chosen = jnp.zeros((tok, tok), F32)
    for j in range(topk_ref.shape[0]):
        chosen = jnp.where(topk_ref[j:j + 1, :] == line, 1.0, chosen)
    before = jnp.where(line < iota((tok, tok), 1), 1.0, 0.0).astype(BF16)
    code_t = jnp.where(chosen > 0.5, dot(chosen.astype(BF16), before), -1.0)
    code_all[me] = code_t[:experts].reshape(group, local, tok)
    code = code_t.T

    gain = gain_ref[...].reshape(1, hid)

    def norm(rows_f32):
        inv_rms = lax.rsqrt(jnp.mean(rows_f32 * rows_f32, axis=-1, keepdims=True) + NORM_EPS)
        return (rows_f32 * inv_rms * gain).astype(BF16)

    x_own = gx[me].astype(F32)
    normed[...] = norm(x_own)
    acc[...] = x_own

    pl.semaphore_wait(barrier, group - 1)

    def code_send(dst, r):
        return pltpu.make_async_remote_copy(
            src_ref=code_all.at[me, dst], dst_ref=code_all.at[me, dst], send_sem=cs_sem.at[r], recv_sem=cr_sem.at[me],
            device_id={"ep": dst}, device_id_type=MESH)

    def code_wait(src):
        pltpu.make_async_remote_copy(
            src_ref=code_all.at[src, me], dst_ref=code_all.at[src, me], send_sem=cs_sem.at[0], recv_sem=cr_sem.at[src],
            device_id={"ep": me}, device_id_type=MESH).wait_recv()

    for r in range(1, group):
        code_send((me + r) % group, r).start()

    def x_send(src, part, dst, slot):
        rows = gx.at[src, pl.ds(part * half, half)]
        return pltpu.make_async_remote_copy(
            src_ref=rows, dst_ref=rows, send_sem=xs_sem.at[slot], recv_sem=xr_sem.at[src, part],
            device_id={"ep": dst}, device_id_type=MESH)

    def x_wait(src, part):
        x_send(src, part, me, 0).wait_recv()

    left, right, far, partner = dev(chips - 1, 0), dev(1, 0), dev(2, 0), dev(0, 1)
    x_sends = [
        (me, 0, right), (me, 1, left), (me, 1, right), (me, 0, left), (me, 0, partner), (me, 1, partner),
        (left, 0, right), (left, 0, partner), (right, 1, left), (right, 1, partner),
        (left, 1, partner), (right, 0, partner), (far, 0, partner), (far, 1, partner),
    ]

    def start_x(lo, hi):
        for slot in range(lo, hi):
            x_send(*x_sends[slot], slot).start()

    start_x(0, 6)

    logits = lax.dot_general(normed[...], rw_ref[...], (((1,), (1,)), ((), ())), preferred_element_type=F32)
    peak = jnp.max(logits, axis=-1, keepdims=True)
    grown = jnp.exp(logits - peak)
    probs = grown / jnp.sum(grown, axis=-1, keepdims=True)
    p_hi = probs.astype(BF16)
    rest = probs - p_hi.astype(F32)
    p_mid = rest.astype(BF16)
    p_low = (rest - p_mid.astype(F32)).astype(BF16)
    spread_in = jnp.concatenate([code[:, :experts].astype(BF16), p_hi, p_mid, p_low], axis=0)

    def slot_weights(i, carry):
        lane = iota((1, group * MAIN), 1)
        owner, place = lane // MAIN, lane % MAIN
        extra = MAIN // local
        last = jnp.full((1, group * MAIN), i, jnp.int32) == local
        expert = owner * local + jnp.where(last, place // extra, i)
        rank = jnp.where(last, MAIN + place % extra, place).astype(F32)
        pick = jnp.where(iota((experts, group * MAIN), 0) == expert, 1.0, 0.0).astype(BF16)
        spread = dot(spread_in, pick)
        hit = spread[:tok] == rank
        for part in range(3):
            value = jnp.where(hit, spread[(part + 1) * tok:(part + 2) * tok], 0.0)
            w_stack[i, pl.ds(part * tok, tok), :] = value.astype(BF16)
        return carry

    lax.fori_loop(0, rounds, slot_weights, 0)

    places = [(0, 0), (0, 1), (1, 0), (1, 1), (chips - 1, 0), (chips - 1, 1), (2, 0), (2, 1)]
    owners = [dev(off, flip) for off, flip in places]
    near = 6
    extra = MAIN // local

    def gather_owner(src, p):
        codes = code_all[src, me]
        spread = jnp.broadcast_to(codes[:, None, :], (local, MAIN, tok)).reshape(local * MAIN, tok)
        place = iota((local * MAIN, tok), 0) % MAIN
        pick = jnp.where(spread == place.astype(F32), 1.0, 0.0).astype(BF16)
        want = jnp.where(place // extra == p, MAIN + place % extra, -2).astype(F32)
        sel_tail[p // 2, :, pl.ds(pl.multiple_of(src % 2 * tok, tok), tok)] = jnp.where(spread == want, 1.0, 0.0).astype(BF16)
        rows = norm(dot(pick, gx[src]))
        xo[:, p] = rows.reshape(local, MAIN, hid)

    def gather_extra(pair):
        first = dev(places[2 * pair][0], 0) // 2 * 2
        return dot(sel_tail[pair], gx[pl.ds(first, 2)].reshape(2 * tok, hid))

    for src in owners[1:]:
        code_wait(src)
    for part in range(2):
        x_wait(partner, part)

    def gather_home(p, carry):
        gather_owner(dev(0, p), p)
        return carry

    lax.fori_loop(0, 2, gather_home, 0)
    x_wait(left, 0)
    start_x(6, 8)
    x_wait(right, 1)
    start_x(8, 10)

    def unit_step(rows, load_rows, gu_first, d_first, put_out, next_gu=None, next_d=None, arrived=False):
        for f in range(FF_CHUNKS):
            slot = (gu_first + f) % GU_SLOTS
            if not arrived:
                for copy in gu_copies(0, 0, slot, False):
                    copy.wait()
            gate = dot(load_rows(), gu_buf[slot, 0])
            up = dot(load_rows(), gu_buf[slot, 1])
            act[pl.ds(0, rows), pl.ds(f * fc, fc)] = (jax.nn.silu(gate) * up).astype(BF16)
            if next_gu is not None:
                next_gu(f, slot)
        for h in range(H_CHUNKS):
            slot = (d_first + h) % D_SLOTS
            if not arrived:
                d_copy(0, 0, slot, False).wait()
            put_out(h, dot(act[pl.ds(0, rows), :], d_buf[slot]))
            if next_d is not None:
                next_d(h, slot)

    def shared_step(u, carry):
        def next_gu(f, slot):
            ahead = (f + GU_SLOTS) // FF_CHUNKS
            f_next = (f + GU_SLOTS) % FF_CHUNKS

            @pl.when(u + ahead < shared_units)
            def _():
                start_gu(u + ahead, f_next, slot, True)

            @pl.when(u + ahead >= shared_units)
            def _():
                start_gu(u + ahead - shared_units, f_next, slot, False)

        def next_d(h, slot):
            d_copy(u + D_SLOTS // H_CHUNKS - shared_units, h, slot, False).start()

        def put_out(h, value):
            cols = pl.ds(h * hc, hc)
            acc[:, cols] = acc[:, cols] + value

        unit_step(tok, lambda: normed[...], u * FF_CHUNKS, u * H_CHUNKS, put_out, next_gu, next_d)

        return carry

    lax.fori_loop(0, shared_units, shared_step, 0)
    x_wait(left, 1)
    start_x(10, 11)
    x_wait(right, 0)
    start_x(11, 12)

    def gather_side(core_flip):
        def step(q, carry):
            gather_owner(dev(1 + q * (chips - 2), core_flip), 2 + 2 * q + core_flip)
            return carry

        lax.fori_loop(0, 2, step, 0)

    gather_side(0)
    for off in (1, chips - 1):
        for part in range(2):
            x_wait(dev(off, 1), part)
    gather_side(1)

    send_order = [6, 7, 2, 4, 3, 5, 1]

    def back_send(i, src_ref, p):
        return pltpu.make_async_remote_copy(
            src_ref=src_ref, dst_ref=back.at[i, me], send_sem=os_sem.at[i, p - 1], recv_sem=or_sem.at[i, me],
            device_id={"ep": owners[p]}, device_id_type=MESH)

    def back_wait(i, src):
        pltpu.make_async_remote_copy(
            src_ref=back.at[i, src], dst_ref=back.at[i, src], send_sem=os_sem.at[0, 0], recv_sem=or_sem.at[i, src],
            device_id={"ep": me}, device_id_type=MESH).wait_recv()

    def combine(i):
        for p in range(1, group):
            back_wait(i, owners[p])
        for h in range(H_CHUNKS):
            cols = pl.ds(h * hc, hc)
            parts = dot(w_stack[i], back[i, :, :, cols].reshape(group * MAIN, hc))
            acc[:, cols] = acc[:, cols] + (parts[:tok] + (parts[tok:2 * tok] + parts[2 * tok:]))

    def next_gu_of(i):
        def next_gu(f, slot):
            ahead = (f + GU_SLOTS) // FF_CHUNKS
            f_next = (f + GU_SLOTS) % FF_CHUNKS

            @pl.when(i + ahead < local)
            def _():
                start_gu(i + ahead, f_next, slot, False)

        return next_gu

    def next_d_of(i):
        def next_d(h, slot):
            ahead = D_SLOTS // H_CHUNKS

            @pl.when(i + ahead < local)
            def _():
                d_copy(i + ahead, h, slot, False).start()

        return next_d

    def expert(i, lo, hi, first_pass, last_pass):
        rows = (hi - lo) * MAIN

        def put_out(h, value):
            xo[i, pl.ds(lo, hi - lo), :, pl.ds(h * hc, hc)] = value.astype(BF16).reshape(hi - lo, MAIN, hc)

        unit_step(
            rows, lambda: xo[i, pl.ds(lo, hi - lo)].reshape(rows, hid),
            (i + shared_units) * FF_CHUNKS, (i + shared_units) * H_CHUNKS, put_out,
            next_gu_of(i) if last_pass else None, next_d_of(i) if last_pass else None, not first_pass)
        for p in send_order:
            if lo <= p < hi:
                back_send(i, xo.at[i, p], p).start()
        if lo == 0:
            back[i, me] = xo[i, 0]

    expert(0, 0, near, True, False)
    tail_sum[...] = gather_extra(0) + gather_extra(1) + gather_extra(2)
    x_wait(far, 0)
    start_x(12, 13)
    x_wait(far, 1)
    start_x(13, 14)
    gather_owner(far, near)
    for part in range(2):
        x_wait(owners[7], part)
    gather_owner(owners[7], near + 1)
    xo[:, group] = norm(tail_sum[...] + gather_extra(3)).reshape(local, MAIN, hid)
    expert(0, near, group + 1, False, True)

    def routed_step(i, carry):
        expert(i, 0, group + 1, True, True)

        @pl.when(i >= 2)
        def _():
            combine(i - 2)

        return carry

    lax.fori_loop(1, local, routed_step, 0)

    left_over = xo[:, group].reshape(local * MAIN, hid)
    row, col = iota((local * MAIN, local * MAIN), 0), iota((local * MAIN, local * MAIN), 1)
    source = ((row % MAIN) // extra) * MAIN + (row // MAIN) * extra + row % extra
    reorder = jnp.where(col == source, 1.0, 0.0).astype(BF16)
    tail[...] = dot(reorder, left_over).astype(BF16).reshape(group, MAIN, hid)
    for p in send_order:
        back_send(local, tail.at[p], p).start()
    back[local, me] = tail[0]

    def combine_step(i, carry):
        combine(i)
        return carry

    lax.fori_loop(local - 2, rounds, combine_step, 0)
    normed[...] = acc[...].astype(BF16)
    out_copy = pltpu.make_async_copy(normed, out_hbm, x_sem)
    out_copy.start()

    for slot in range(len(x_sends)):
        x_send(*x_sends[slot], slot).wait_send()
    for r in range(1, group):
        code_send((me + r) % group, r).wait_send()

    def drain(i, carry):
        for p in send_order:
            back_send(i, tail.at[p], p).wait_send()
        return carry

    lax.fori_loop(0, rounds, drain, 0)
    out_copy.wait()


def solution(mesh):
    group = mesh.shape["ep"]

    def local_step(hidden, norm_gain, router_w, topk_idx, w_gate, w_up, w_down, shared_gate, shared_up, shared_down):
        tok, hid = hidden.shape
        top_k = topk_idx.shape[1]
        experts = router_w.shape[1]
        local, _, ff = w_gate.shape
        capacity = 3 * tok * top_k // (2 * experts)
        assert group == 8 and (capacity - MAIN) * local == MAIN and local == group
        rounds = local + 1
        fc, hc = ff // FF_CHUNKS, hid // H_CHUNKS
        any_spec = pl.BlockSpec(memory_space=pl.ANY)
        dma = pltpu.SemaphoreType.DMA
        return pl.pallas_call(
            functools.partial(moe_kernel, group),
            out_shape=jax.ShapeDtypeStruct((tok, hid), BF16),
            in_specs=[any_spec] * 10,
            out_specs=any_spec,
            scratch_shapes=[
                pltpu.VMEM((group, tok, hid), BF16),
                pltpu.VMEM((local, group + 1, MAIN, hid), BF16),
                pltpu.VMEM((rounds, group, MAIN, hid), BF16),
                pltpu.VMEM((group, MAIN, hid), BF16),
                pltpu.VMEM((GU_SLOTS, 2, hid, fc), BF16),
                pltpu.VMEM((D_SLOTS, ff, hc), BF16),
                pltpu.VMEM(((group + 1) * MAIN, ff), BF16),
                pltpu.VMEM((tok, hid), BF16),
                pltpu.VMEM((tok, hid), F32),
                pltpu.VMEM((rounds, 3 * tok, group * MAIN), BF16),
                pltpu.VMEM((group, group, local, tok), F32),
                pltpu.VMEM((group // 2, local * MAIN, 2 * tok), BF16),
                pltpu.VMEM((local * MAIN, hid), F32),
                pltpu.VMEM((hid,), F32),
                pltpu.VMEM((experts, hid), BF16),
                pltpu.VMEM((top_k, tok), jnp.int32),
                dma((3,)),
                dma,
                dma((GU_SLOTS, 2)),
                dma((D_SLOTS,)),
                dma((14,)),
                dma((group, 2)),
                dma((group,)),
                dma((group,)),
                dma((rounds, group - 1)),
                dma((rounds, group)),
            ],
            compiler_params=pltpu.CompilerParams(
                collective_id=0, has_side_effects=True, vmem_limit_bytes=67_000_000),
            name="moe_block",
        )(hidden, norm_gain, router_w.T, topk_idx.T, w_gate, w_up, w_down, shared_gate, shared_up, shared_down)

    token_spec = P(("dp", "ep"), None)
    expert_spec = P("ep", None, None)
    return jax.shard_map(
        local_step,
        mesh=mesh,
        in_specs=(token_spec, P(None), P(None, None), token_spec, expert_spec, expert_spec, expert_spec,
                  P(None, None), P(None, None), P(None, None)),
        out_specs=token_spec,
        check_vma=False,
    )
```

```python
import functools

import jax
import jax.numpy as jnp
from jax import lax
from jax.experimental import pallas as pl
from jax.experimental.pallas import tpu as pltpu
from jax.sharding import PartitionSpec as P

NORM_EPS = 1e-6
MESH = pl.DeviceIdType.MESH
F32 = jnp.float32
BF16 = jnp.bfloat16
MAIN = 16
GU_SLOTS = 4
D_SLOTS = 4
FF_CHUNKS = 3
H_CHUNKS = 2
EARLY = 1


def dot(a, b):
    return jnp.dot(a, b, preferred_element_type=F32)


def iota(shape, axis):
    return lax.broadcasted_iota(jnp.int32, shape, axis)


def moe_kernel(
    group, x_hbm, gain_hbm, rw_hbm, topk_hbm, wg, wu, wd, sg, su, sd, out_hbm,
    gx, xo, back, tail, gu_buf, d_buf, act, normed, acc, w_stack, code_all, sel_tail, tail_sum,
    gain_ref, rw_ref, topk_ref, in_sem, x_sem, gu_sem, d_sem, xs_sem, xr_sem, cs_sem, cr_sem, os_sem, or_sem,
):
    tok, hid = x_hbm.shape
    ff = wg.shape[2]
    local = wg.shape[0]
    experts = rw_hbm.shape[0]
    rounds = local + 1
    fc, hc = ff // FF_CHUNKS, hid // H_CHUNKS
    shared_units = sg.shape[1] // ff
    half = tok // 2
    chips = group // 2

    me = lax.axis_index("ep")
    chip, core = me // 2, me % 2

    def dev(chip_off, flip):
        return ((chip + chip_off) % chips) * 2 + (core + flip) % 2

    def gu_copies(unit, f, slot, shared):
        if shared:
            cols = pl.ds(pl.multiple_of(unit * ff + f * fc, 128), fc)
            srcs = (sg.at[:, cols], su.at[:, cols])
        else:
            cols = pl.ds(f * fc, fc)
            srcs = (wg.at[unit, :, cols], wu.at[unit, :, cols])
        return [pltpu.make_async_copy(srcs[m], gu_buf.at[slot, m], gu_sem.at[slot, m]) for m in range(2)]

    def d_copy(unit, h, slot, shared):
        cols = pl.ds(h * hc, hc)
        src = sd.at[pl.ds(pl.multiple_of(unit * ff, 16), ff), cols] if shared else wd.at[unit, :, cols]
        return pltpu.make_async_copy(src, d_buf.at[slot], d_sem.at[slot])

    def start_gu(unit, f, slot, shared):
        for copy in gu_copies(unit, f, slot, shared):
            copy.start()

    x_copy = pltpu.make_async_copy(x_hbm, gx.at[me], x_sem)
    x_copy.start()
    small = [
        pltpu.make_async_copy(topk_hbm, topk_ref, in_sem.at[0]),
        pltpu.make_async_copy(gain_hbm, gain_ref, in_sem.at[1]),
        pltpu.make_async_copy(rw_hbm, rw_ref, in_sem.at[2]),
    ]
    for copy in small:
        copy.start()

    barrier = pltpu.get_barrier_semaphore()
    for r in range(1, group):
        pl.semaphore_signal(barrier, inc=1, device_id={"ep": (me + r) % group}, device_id_type=MESH)
    x_copy.wait()
    for q in range(FF_CHUNKS):
        start_gu(0, q, q, True)
    for q in range(H_CHUNKS):
        d_copy(0, q, q, True).start()

    for copy in small:
        copy.wait()
    line = iota((tok, tok), 0)
    chosen = jnp.zeros((tok, tok), F32)
    for j in range(topk_ref.shape[0]):
        chosen = jnp.where(topk_ref[j:j + 1, :] == line, 1.0, chosen)
    before = jnp.where(line < iota((tok, tok), 1), 1.0, 0.0).astype(BF16)
    code_t = jnp.where(chosen > 0.5, dot(chosen.astype(BF16), before), -1.0)
    code_all[me] = code_t[:experts].reshape(group, local, tok)
    code = code_t.T

    gain = gain_ref[...].reshape(1, hid)

    def norm(rows_f32):
        inv_rms = lax.rsqrt(jnp.mean(rows_f32 * rows_f32, axis=-1, keepdims=True) + NORM_EPS)
        return (rows_f32 * inv_rms * gain).astype(BF16)

    x_own = gx[me].astype(F32)
    normed[...] = norm(x_own)
    acc[...] = x_own

    pl.semaphore_wait(barrier, group - 1)

    def code_send(dst, r):
        return pltpu.make_async_remote_copy(
            src_ref=code_all.at[me, dst], dst_ref=code_all.at[me, dst], send_sem=cs_sem.at[r], recv_sem=cr_sem.at[me],
            device_id={"ep": dst}, device_id_type=MESH)

    def code_wait(src):
        pltpu.make_async_remote_copy(
            src_ref=code_all.at[src, me], dst_ref=code_all.at[src, me], send_sem=cs_sem.at[0], recv_sem=cr_sem.at[src],
            device_id={"ep": me}, device_id_type=MESH).wait_recv()

    for r in range(1, group):
        code_send((me + r) % group, r).start()

    def x_send(src, part, dst, slot):
        rows = gx.at[src, pl.ds(part * half, half)]
        return pltpu.make_async_remote_copy(
            src_ref=rows, dst_ref=rows, send_sem=xs_sem.at[slot], recv_sem=xr_sem.at[src, part],
            device_id={"ep": dst}, device_id_type=MESH)

    def x_wait(src, part):
        x_send(src, part, me, 0).wait_recv()

    left, right, far, partner = dev(chips - 1, 0), dev(1, 0), dev(2, 0), dev(0, 1)
    x_sends = [
        (me, 0, right), (me, 1, left), (me, 1, right), (me, 0, left), (me, 0, partner), (me, 1, partner),
        (left, 0, right), (left, 0, partner), (right, 1, left), (right, 1, partner),
        (left, 1, partner), (right, 0, partner), (far, 0, partner), (far, 1, partner),
    ]

    def start_x(lo, hi):
        for slot in range(lo, hi):
            x_send(*x_sends[slot], slot).start()

    start_x(0, 6)
    for q in range(FF_CHUNKS, GU_SLOTS):
        start_gu(q // FF_CHUNKS - EARLY, q % FF_CHUNKS, q, False)
    for q in range(H_CHUNKS, D_SLOTS):
        d_copy(q // H_CHUNKS - EARLY, q % H_CHUNKS, q, False).start()

    logits = lax.dot_general(normed[...], rw_ref[...], (((1,), (1,)), ((), ())), preferred_element_type=F32)
    peak = jnp.max(logits, axis=-1, keepdims=True)
    grown = jnp.exp(logits - peak)
    probs = grown / jnp.sum(grown, axis=-1, keepdims=True)
    p_hi = probs.astype(BF16)
    rest = probs - p_hi.astype(F32)
    p_mid = rest.astype(BF16)
    p_low = (rest - p_mid.astype(F32)).astype(BF16)
    spread_in = jnp.concatenate([code[:, :experts].astype(BF16), p_hi, p_mid, p_low], axis=0)

    def slot_weights(i, carry):
        lane = iota((1, group * MAIN), 1)
        owner, place = lane // MAIN, lane % MAIN
        extra = MAIN // local
        last = jnp.full((1, group * MAIN), i, jnp.int32) == local
        expert = owner * local + jnp.where(last, place // extra, i)
        rank = jnp.where(last, MAIN + place % extra, place).astype(F32)
        pick = jnp.where(iota((experts, group * MAIN), 0) == expert, 1.0, 0.0).astype(BF16)
        spread = dot(spread_in, pick)
        hit = spread[:tok] == rank
        for part in range(3):
            value = jnp.where(hit, spread[(part + 1) * tok:(part + 2) * tok], 0.0)
            w_stack[i, pl.ds(part * tok, tok), :] = value.astype(BF16)
        return carry

    lax.fori_loop(0, rounds, slot_weights, 0)

    places = [(0, 0), (0, 1), (1, 0), (1, 1), (chips - 1, 0), (chips - 1, 1), (2, 0), (2, 1)]
    owners = [dev(off, flip) for off, flip in places]
    near = 6
    extra = MAIN // local

    def gather_owner(src, p):
        codes = code_all[src, me]
        spread = jnp.broadcast_to(codes[:, None, :], (local, MAIN, tok)).reshape(local * MAIN, tok)
        place = iota((local * MAIN, tok), 0) % MAIN
        pick = jnp.where(spread == place.astype(F32), 1.0, 0.0).astype(BF16)
        want = jnp.where(place // extra == p, MAIN + place % extra, -2).astype(F32)
        sel_tail[p // 2, :, pl.ds(pl.multiple_of(src % 2 * tok, tok), tok)] = jnp.where(spread == want, 1.0, 0.0).astype(BF16)
        rows = norm(dot(pick, gx[src]))
        xo[:, p] = rows.reshape(local, MAIN, hid)

    def gather_extra(pair):
        first = dev(places[2 * pair][0], 0) // 2 * 2
        return dot(sel_tail[pair], gx[pl.ds(first, 2)].reshape(2 * tok, hid))

    for src in owners[1:]:
        code_wait(src)
    for part in range(2):
        x_wait(partner, part)

    def gather_home(p, carry):
        gather_owner(dev(0, p), p)
        return carry

    lax.fori_loop(0, 2, gather_home, 0)
    def unit_step(rows, load_rows, gu_first, d_first, put_out, next_gu=None, next_d=None, arrived=False):
        for f in range(FF_CHUNKS):
            slot = (gu_first + f) % GU_SLOTS
            if not arrived:
                for copy in gu_copies(0, 0, slot, False):
                    copy.wait()
            gate = dot(load_rows(), gu_buf[slot, 0])
            up = dot(load_rows(), gu_buf[slot, 1])
            act[pl.ds(0, rows), pl.ds(f * fc, fc)] = (jax.nn.silu(gate) * up).astype(BF16)
            if next_gu is not None:
                next_gu(f, slot)
        for h in range(H_CHUNKS):
            slot = (d_first + h) % D_SLOTS
            if not arrived:
                d_copy(0, 0, slot, False).wait()
            put_out(h, dot(act[pl.ds(0, rows), :], d_buf[slot]))
            if next_d is not None:
                next_d(h, slot)

    def next_gu_of(n):
        def next_gu(f, slot):
            unit = n + (f + GU_SLOTS) // FF_CHUNKS
            f_next = (f + GU_SLOTS) % FF_CHUNKS

            @pl.when(unit < local + EARLY)
            def _():
                start_gu(unit - EARLY, f_next, slot, False)

            @pl.when((unit >= local + EARLY) & (unit < local + shared_units))
            def _():
                start_gu(unit - local, f_next, slot, True)

        return next_gu

    def next_d_of(n):
        def next_d(h, slot):
            unit = n + D_SLOTS // H_CHUNKS

            @pl.when(unit < local + EARLY)
            def _():
                d_copy(unit - EARLY, h, slot, False).start()

            @pl.when((unit >= local + EARLY) & (unit < local + shared_units))
            def _():
                d_copy(unit - local, h, slot, True).start()

        return next_d

    def shared_unit(n):
        def put_out(h, value):
            cols = pl.ds(h * hc, hc)
            acc[:, cols] = acc[:, cols] + value

        unit_step(tok, lambda: normed[...], n * FF_CHUNKS, n * H_CHUNKS, put_out, next_gu_of(n), next_d_of(n))

    for n in range(EARLY):
        shared_unit(n)
    x_wait(left, 0)
    start_x(6, 8)
    x_wait(right, 1)
    start_x(8, 10)
    x_wait(left, 1)
    start_x(10, 11)
    x_wait(right, 0)
    start_x(11, 12)

    def gather_side(core_flip):
        def step(q, carry):
            gather_owner(dev(1 + q * (chips - 2), core_flip), 2 + 2 * q + core_flip)
            return carry

        lax.fori_loop(0, 2, step, 0)

    gather_side(0)
    for off in (1, chips - 1):
        for part in range(2):
            x_wait(dev(off, 1), part)
    gather_side(1)

    send_order = [6, 7, 2, 4, 3, 5, 1]

    def back_send(i, src_ref, p):
        return pltpu.make_async_remote_copy(
            src_ref=src_ref, dst_ref=back.at[i, me], send_sem=os_sem.at[i, p - 1], recv_sem=or_sem.at[i, me],
            device_id={"ep": owners[p]}, device_id_type=MESH)

    def back_wait(i, src):
        pltpu.make_async_remote_copy(
            src_ref=back.at[i, src], dst_ref=back.at[i, src], send_sem=os_sem.at[0, 0], recv_sem=or_sem.at[i, src],
            device_id={"ep": me}, device_id_type=MESH).wait_recv()

    def combine(i):
        for p in range(1, group):
            back_wait(i, owners[p])
        for h in range(H_CHUNKS):
            cols = pl.ds(h * hc, hc)
            parts = dot(w_stack[i], back[i, :, :, cols].reshape(group * MAIN, hc))
            acc[:, cols] = acc[:, cols] + (parts[:tok] + (parts[tok:2 * tok] + parts[2 * tok:]))

    def expert(i, lo, hi, first_pass, last_pass):
        rows = (hi - lo) * MAIN
        n = i + EARLY

        def put_out(h, value):
            xo[i, pl.ds(lo, hi - lo), :, pl.ds(h * hc, hc)] = value.astype(BF16).reshape(hi - lo, MAIN, hc)

        unit_step(
            rows, lambda: xo[i, pl.ds(lo, hi - lo)].reshape(rows, hid),
            n * FF_CHUNKS, n * H_CHUNKS, put_out,
            next_gu_of(n) if last_pass else None, next_d_of(n) if last_pass else None, not first_pass)
        for p in send_order:
            if lo <= p < hi:
                back_send(i, xo.at[i, p], p).start()
        if lo == 0:
            back[i, me] = xo[i, 0]

    expert(0, 0, near, True, False)
    tail_sum[...] = gather_extra(0) + gather_extra(1) + gather_extra(2)
    x_wait(far, 0)
    start_x(12, 13)
    x_wait(far, 1)
    start_x(13, 14)
    gather_owner(far, near)
    for part in range(2):
        x_wait(owners[7], part)
    gather_owner(owners[7], near + 1)
    xo[:, group] = norm(tail_sum[...] + gather_extra(3)).reshape(local, MAIN, hid)
    expert(0, near, group + 1, False, True)

    lag = 3

    def routed_step(i, carry):
        expert(i, 0, group + 1, True, True)

        @pl.when(i >= lag)
        def _():
            combine(i - lag)

        return carry

    lax.fori_loop(1, local, routed_step, 0)

    left_over = xo[:, group].reshape(local * MAIN, hid)
    row, col = iota((local * MAIN, local * MAIN), 0), iota((local * MAIN, local * MAIN), 1)
    source = ((row % MAIN) // extra) * MAIN + (row // MAIN) * extra + row % extra
    reorder = jnp.where(col == source, 1.0, 0.0).astype(BF16)
    tail[...] = dot(reorder, left_over).astype(BF16).reshape(group, MAIN, hid)
    for p in send_order:
        back_send(local, tail.at[p], p).start()
    back[local, me] = tail[0]

    for n in range(local + EARLY, local + shared_units):
        shared_unit(n)

    def combine_step(i, carry):
        combine(i)
        return carry

    lax.fori_loop(local - lag, rounds, combine_step, 0)
    normed[...] = acc[...].astype(BF16)
    out_copy = pltpu.make_async_copy(normed, out_hbm, x_sem)
    out_copy.start()

    for slot in range(len(x_sends)):
        x_send(*x_sends[slot], slot).wait_send()
    for r in range(1, group):
        code_send((me + r) % group, r).wait_send()

    def drain(i, carry):
        for p in send_order:
            back_send(i, tail.at[p], p).wait_send()
        return carry

    lax.fori_loop(0, rounds, drain, 0)
    out_copy.wait()


def solution(mesh):
    group = mesh.shape["ep"]

    def local_step(hidden, norm_gain, router_w, topk_idx, w_gate, w_up, w_down, shared_gate, shared_up, shared_down):
        tok, hid = hidden.shape
        top_k = topk_idx.shape[1]
        experts = router_w.shape[1]
        local, _, ff = w_gate.shape
        capacity = 3 * tok * top_k // (2 * experts)
        assert group == 8 and (capacity - MAIN) * local == MAIN and local == group
        rounds = local + 1
        fc, hc = ff // FF_CHUNKS, hid // H_CHUNKS
        any_spec = pl.BlockSpec(memory_space=pl.ANY)
        dma = pltpu.SemaphoreType.DMA
        return pl.pallas_call(
            functools.partial(moe_kernel, group),
            out_shape=jax.ShapeDtypeStruct((tok, hid), BF16),
            in_specs=[any_spec] * 10,
            out_specs=any_spec,
            scratch_shapes=[
                pltpu.VMEM((group, tok, hid), BF16),
                pltpu.VMEM((local, group + 1, MAIN, hid), BF16),
                pltpu.VMEM((rounds, group, MAIN, hid), BF16),
                pltpu.VMEM((group, MAIN, hid), BF16),
                pltpu.VMEM((GU_SLOTS, 2, hid, fc), BF16),
                pltpu.VMEM((D_SLOTS, ff, hc), BF16),
                pltpu.VMEM(((group + 1) * MAIN, ff), BF16),
                pltpu.VMEM((tok, hid), BF16),
                pltpu.VMEM((tok, hid), F32),
                pltpu.VMEM((rounds, 3 * tok, group * MAIN), BF16),
                pltpu.VMEM((group, group, local, tok), F32),
                pltpu.VMEM((group // 2, local * MAIN, 2 * tok), BF16),
                pltpu.VMEM((local * MAIN, hid), F32),
                pltpu.VMEM((hid,), F32),
                pltpu.VMEM((experts, hid), BF16),
                pltpu.VMEM((top_k, tok), jnp.int32),
                dma((3,)),
                dma,
                dma((GU_SLOTS, 2)),
                dma((D_SLOTS,)),
                dma((14,)),
                dma((group, 2)),
                dma((group,)),
                dma((group,)),
                dma((rounds, group - 1)),
                dma((rounds, group)),
            ],
            compiler_params=pltpu.CompilerParams(
                collective_id=0, has_side_effects=True, vmem_limit_bytes=67_000_000),
            name="moe_block",
        )(hidden, norm_gain, router_w.T, topk_idx.T, w_gate, w_up, w_down, shared_gate, shared_up, shared_down)

    token_spec = P(("dp", "ep"), None)
    expert_spec = P("ep", None, None)
    return jax.shard_map(
        local_step,
        mesh=mesh,
        in_specs=(token_spec, P(None), P(None, None), token_spec, expert_spec, expert_spec, expert_spec,
                  P(None, None), P(None, None), P(None, None)),
        out_specs=token_spec,
        check_vma=False,
    )
```
